32 devices in a mesh: row: 8 (over z, x), col: 4 (over y, core).
Axes of the slice: x: 2, y: 2, z: 4, core: 2. Of those that a mesh axis runs over, the one named last changes fastest.
Arguments:
- acquired_tiles: bfloat16 [4, 32768, 1024], P(None, ('row', 'col')), may hold values from -24 to 24
- row_live: int32 [4, 32768], P(None, ('row', 'col')), may hold values from 0 to 1, as said below
- col_live: int32 [4, 32768], P(None, ('row', 'col')), may hold values 0 or 1
- row_order: int32 [8], replicated, may hold values from 0 to 7, as said below
- source_init: float32 [32768, 256], P(('row', 'col')), may hold values from -3 to 3
- receiver_init: float32 [32768, 256], P(('row', 'col')), may hold values from -3 to 3
Outputs:
- sources: float32 [32768, 256], P(('row', 'col'))
- receivers: float32 [32768, 256], P(('row', 'col'))
The draws below stay inside these ranges and needn't reach their ends.
Inputs may be any that keep to these rules, and one draw needn't show every extreme that they name: `row_live`: 1 where the source of that row is recorded in that stratum's tile; sources go missing singly and in whole aligned lines of 128 rows, and the share of missing lines differs from block to block. `row_order`: each number once.
All inputs are finite; a program needn't handle non-finite values. No bound on the sum of `col_live` on one device may be relied on, other than what follows from the above.
Results may differ from the reference program's by a relative error of at most 0.00096.
Values sent between devices are 32-bit elements; how exact they have to be, the bound alone decides.
A program may use at most 128 MiB of HBM per device.

```python
import jax
import jax.numpy as jnp
from jax import lax

K = 256
BLOCK = 1024
BAND = 128
STRATA = 4
STEPS = 2
ORDER = 32768
N_ROW = 8
N_COL = 4
DEVICES = 32


def draw_row_live(key, part):
    seeded = jax.random.fold_in(key, 7)
    first_key, second_key = jax.random.split(seeded)
    band_total = ORDER // BAND
    owner_block = jnp.arange(band_total, dtype=jnp.int32) * BAND // BLOCK
    threshold = owner_block * 7 // DEVICES
    band_draw = jax.random.randint(first_key, (STRATA, band_total), 0, 10)
    band_live = (band_draw >= threshold[None, :]).astype(jnp.int32)
    single = (jax.random.randint(second_key, (STRATA, ORDER), 0, 5) > 0).astype(jnp.int32)
    return jnp.repeat(band_live, BAND, axis=1) * single


def draw_row_order(key, part):
    seeded = jax.random.fold_in(key, 17)
    perm_key, pick_key = jax.random.split(seeded)
    shuffled = jax.random.permutation(perm_key, N_ROW).astype(jnp.int32)
    chosen = jax.random.randint(pick_key, (), 0, N_ROW).astype(jnp.int32)
    wanted = (chosen + N_ROW - 1) % N_ROW
    positions = jnp.arange(N_ROW, dtype=jnp.int32)
    holder = jnp.sum(jnp.where(shuffled == wanted, positions, 0)).astype(jnp.int32)
    displaced = jnp.sum(jnp.where(positions == chosen, shuffled, 0)).astype(jnp.int32)
    result = jnp.where(positions == holder, displaced, shuffled)
    result = jnp.where(positions == chosen, wanted, result)
    return result.astype(jnp.int32)


def factor_draw(key, salt):
    seeded = jax.random.fold_in(key, salt)
    base_key = jax.random.fold_in(seeded, 0)
    values = 0.5 * jax.random.normal(base_key, (ORDER, K), jnp.float32)
    return jnp.clip(values, -3.0, 3.0)


def draw_source_init(key, part):
    return factor_draw(key, 11)


def draw_receiver_init(key, part):
    return factor_draw(key, 13)


def place_ends(drawn, rng, low, largest):
    index_at = [jax.random.randint(jax.random.fold_in(rng, axis), (), 0, length) for axis, length in enumerate(drawn.shape)]
    widest = drawn.shape.index(max(drawn.shape))
    neighbour = index_at[:widest] + [(index_at[widest] + 1) % drawn.shape[widest]] + index_at[widest + 1:]
    return drawn.at[tuple(index_at)].set(low).at[tuple(neighbour)].set(largest)


def steps_of(key, extent, pieces, smallest, top_value):
    loudness, own = 1.0, jax.random.fold_in(key, 6)
    for dim, parts in pieces:
        draws = jnp.exp(jax.random.uniform(jax.random.fold_in(own, dim), (parts,), jnp.float32, smallest / len(pieces), top_value / len(pieces)))
        loudness = loudness * jnp.repeat(draws, extent[dim] // parts).reshape([-1 if axis == dim else 1 for axis in range(len(extent))])
    return loudness


def scatter_about(own_key, shape, width, most, cuts=(), kind=jnp.bfloat16):
    level = steps_of(own_key, shape, cuts, -0.22, 0.18) if cuts else 1.0
    entries = jax.random.normal(own_key, shape, jnp.float32) * width * level
    return jnp.minimum(jnp.maximum(entries, -most), most).astype(kind)


def setup_inputs(seed: int = 0) -> dict:
    key_list = jax.random.split(jax.random.key(seed), 7)
    return {
        "acquired_tiles": scatter_about(key_list[0], (STRATA, ORDER, BLOCK), 4.0, 24.0, ((1, 32),)),
        "row_live": draw_row_live(jax.random.fold_in(key_list[6], 71), 0),
        "col_live": place_ends((jax.random.randint(key_list[2], (STRATA, ORDER), 0, 4) < 3).astype(jnp.int32), jax.random.fold_in(key_list[2], 1), 0, 1),
        "row_order": draw_row_order(jax.random.fold_in(key_list[6], 71), 0),
        "source_init": draw_source_init(jax.random.fold_in(key_list[6], 71), 0),
        "receiver_init": draw_receiver_init(jax.random.fold_in(key_list[6], 71), 0),
    }


def fit_block(src_block, rec_block, acquired, live_rows, live_cols):
    weights = live_rows.astype(jnp.float32)[:, None] * live_cols.astype(jnp.float32)[None, :]
    observed = acquired.astype(jnp.float32)
    step_size = 1.0 / (BLOCK + 2 * K)
    for iteration in range(STEPS):
        src_half = src_block.astype(jnp.bfloat16)
        rec_half = rec_block.astype(jnp.bfloat16)
        predicted = jnp.dot(src_half, rec_half.T, preferred_element_type=jnp.float32)
        misfit = (weights * (observed - predicted)).astype(jnp.bfloat16)
        grad_src = jnp.dot(misfit, rec_half, preferred_element_type=jnp.float32)
        grad_rec = jnp.dot(misfit.T, src_half, preferred_element_type=jnp.float32)
        src_block = src_block + step_size * grad_src
        rec_block = rec_block + step_size * grad_rec
    return src_block, rec_block


def reference(acquired_tiles, row_live, col_live, row_order, source_init, receiver_init):
    block_count = ORDER // BLOCK
    src_blocks = source_init.reshape(block_count, BLOCK, K)
    rec_blocks = receiver_init.reshape(block_count, BLOCK, K)
    for stratum in range(STRATA):
        slab_data = acquired_tiles[stratum].reshape(block_count, BLOCK, BLOCK)
        live_rows = row_live[stratum].reshape(block_count, BLOCK)
        live_cols = col_live[stratum].reshape(block_count, BLOCK)
        src_blocks, rec_blocks = lax.map(lambda packed: fit_block(*packed), (src_blocks, rec_blocks, slab_data, live_rows, live_cols))
        if stratum + 1 < STRATA:
            rec_blocks = jnp.roll(rec_blocks, 1, axis=0)
            if stratum == 1:
                rec_blocks = rec_blocks.reshape(N_ROW, N_COL, BLOCK, K)[row_order].reshape(block_count, BLOCK, K)
    return src_blocks.reshape(ORDER, K), rec_blocks.reshape(ORDER, K)
```

```python
import functools

import jax
import jax.numpy as jnp
from jax import lax
from jax.experimental import pallas as pl
from jax.experimental.pallas import tpu as pltpu
from jax.sharding import PartitionSpec as P

STEPS = 2
CHUNKS = 4
MESH = pl.DeviceIdType.MESH
F32 = jnp.float32
BF16 = jnp.bfloat16
LANES = 128


def rounded_sources(src, lanes, half, half_t):
    half[...] = src[...].astype(BF16)
    half_t[...] = (src[...].T * lanes).astype(BF16)


def row_scale(lanes, row_mask, step_size):
    block = row_mask.shape[0]
    for t in range(block // LANES):
        part = slice(t * LANES, (t + 1) * LANES)
        row_mask[part, :] = jnp.broadcast_to(lanes[:, part], (LANES, LANES)).T * step_size


def misfit_of(half, rec_half, observed):
    predicted = jnp.dot(half[...], rec_half, preferred_element_type=F32)
    return (observed.astype(F32) - predicted).astype(BF16)


def source_gradient(misfit, rec_half, live):
    return lax.dot_general(
        misfit, rec_half * live.astype(BF16), (((1,), (1,)), ((), ())),
        preferred_element_type=F32,
    )


def add_sources(dst, src, row_mask, grad):
    for h in range(src.shape[1] // LANES):
        part = slice(h * LANES, (h + 1) * LANES)
        dst[:, part] = src[:, part] + row_mask[...] * grad[:, part]


def sweep(rec_in, rec_out, observed, live_of, half, half_t, grad, step_size, done=None):
    rank, chunk = half_t.shape[0], rec_in.shape[1]
    chunks = rec_in.shape[0] // rank

    def front(q):
        rec_half = rec_in[q * rank:(q + 1) * rank, :].astype(BF16)
        return rec_half, misfit_of(half, rec_half, observed[:, q * chunk:(q + 1) * chunk])

    ahead = front(0)
    for q in range(chunks):
        rec_half, misfit = ahead
        if q + 1 < chunks:
            ahead = front(q + 1)
        rows = slice(q * rank, (q + 1) * rank)
        live = live_of(q)
        grad_rec = jnp.dot(half_t[...], misfit, preferred_element_type=F32)
        rec_out[rows, :] = rec_in[rows, :] + (step_size * live) * grad_rec
        grad_src = source_gradient(misfit, rec_half, live)
        if q == 0:
            grad[...] = grad_src
        else:
            grad[...] += grad_src
        if done is not None:
            done(q)


def main_kernel(nr, nc, tiles, row_live, col_live, order, src_in, rec_in, src_out, rec_out, tile_out,
                tile, rb, mids, outs, stage, grad, half, half_t, row_mask,
                in_sem, ring_send, ring_recv, a_send, a_recv, b_send, b_recv):
    strata, block, width = tiles.shape
    rank = src_out.shape[1]
    chunk = rb.shape[2]
    chunks = width // chunk
    sub = rank // nr
    step_size = 1.0 / (width + 2 * rank)
    r = lax.axis_index("row")
    c = lax.axis_index("col")
    cn = lax.rem(c + 1, nc)
    rn = lax.rem(r + (c + 1) // nc, nr)
    cp = lax.rem(c + nc - 1, nc)

    tile_of = [tile.at[s] for s in range(strata - 1)] + [tile_out]
    loads = [
        pltpu.make_async_copy(rec_in, stage, in_sem.at[strata]),
        pltpu.make_async_copy(src_in, src_out, in_sem.at[strata + 1]),
    ] + [pltpu.make_async_copy(tiles.at[s], tile_of[s], in_sem.at[s]) for s in range(strata)]
    for load in loads:
        load.start()

    barrier = pltpu.get_barrier_semaphore()
    for k in range(nr):
        pl.semaphore_signal(barrier, inc=1, device_id={"row": k, "col": cp}, device_id_type=MESH)
    for k in range(1, nr):
        pl.semaphore_signal(
            barrier, inc=1, device_id={"row": lax.rem(r + k, nr), "col": c}, device_id_type=MESH
        )

    def ring_copy(s, q):
        lane = 0 if s == 0 else 1
        rows = pl.ds(q * rank, rank)
        return pltpu.make_async_remote_copy(
            src_ref=rb.at[s, rows], dst_ref=rb.at[s + 1, rows],
            send_sem=ring_send.at[lane, q], recv_sem=ring_recv.at[lane, q],
            device_id={"row": rn, "col": cn}, device_id_type=MESH,
        )

    def a_copy(q, p, slot, static_q):
        return pltpu.make_async_remote_copy(
            src_ref=rb.at[1, pl.ds(q * rank + p * sub, sub)], dst_ref=mids[static_q].at[slot],
            send_sem=a_send.at[static_q, p], recv_sem=a_recv.at[static_q, slot],
            device_id={"row": p, "col": cn}, device_id_type=MESH,
        )

    def b_copy(q, to, p):
        return pltpu.make_async_remote_copy(
            src_ref=outs.at[q, to], dst_ref=rb.at[2, pl.ds(q * rank + p * sub, sub)],
            send_sem=b_send.at[q, to], recv_sem=b_recv.at[q, p],
            device_id={"row": to, "col": c}, device_id_type=MESH,
        )

    loads[0].wait()
    for q in range(chunks):
        rb[0, q * rank:(q + 1) * rank, :] = stage[q * chunk:(q + 1) * chunk, :].T
    loads[1].wait()

    for s in range(strata):
        lanes = row_live[s:s + 1, :].astype(F32)
        row_scale(lanes, row_mask, step_size)
        loads[s + 2].wait()
        for it in range(STEPS if s + 1 < strata else STEPS - 1):
            rounded_sources(src_out, lanes, half, half_t)

            def one(q, s=s, it=it):
                rows = pl.ds(pl.multiple_of(q * rank, rank), rank)
                cols = pl.ds(pl.multiple_of(q * chunk, chunk), chunk)
                if it == 0 and s == 2:
                    def wait_b(k, carry):
                        b_copy(q, r, lax.rem(r + k, nr)).wait_recv()
                        return carry
                    lax.fori_loop(1, nr, wait_b, 0)
                elif it == 0:
                    ring_copy(s - 1, q).wait_recv()
                rec = rb[s, rows, :]
                rec_half = rec.astype(BF16)
                live = col_live[s:s + 1, cols].astype(F32)
                misfit = misfit_of(half, rec_half, tile_of[s][:, cols])
                grad_rec = jnp.dot(half_t[...], misfit, preferred_element_type=F32)
                updated = rec + (step_size * live) * grad_rec
                if s + 1 == strata:
                    rec_out[rows, :] = updated
                else:
                    rb[s, rows, :] = updated
                grad_src = source_gradient(misfit, rec_half, live)

                @pl.when(q == 0)
                def _():
                    grad[...] = grad_src

                @pl.when(q > 0)
                def _():
                    grad[...] += grad_src

                if it == STEPS - 1 and s in (0, 2):
                    ring_copy(s, q).start()
                if it == STEPS - 1 and s == 1:
                    for static_q in range(chunks):
                        @pl.when(q == static_q)
                        def _(static_q=static_q):
                            def send_a(k, carry):
                                a_copy(static_q, lax.rem(r + k, nr), rn, static_q).start()
                                return carry
                            lax.fori_loop(0, nr, send_a, 0)

            if it == STEPS - 1 and s == 0:
                pl.semaphore_wait(barrier, 2 * nr - 1)
            if it == 0 and s == 0:
                sweep(rb.at[0], rb.at[0], tile_of[0],
                      lambda q: col_live[0:1, q * chunk:(q + 1) * chunk].astype(F32),
                      half, half_t, grad, step_size)
            else:
                def body(q, carry):
                    one(q)
                    return carry
                lax.fori_loop(0, chunks, body, 0)
            add_sources(src_out, src_out, row_mask, grad)
        if s == 1:
            for q in range(chunks):
                def wait_a(k, carry, q=q):
                    a_copy(q, 0, k, q).wait_recv()
                    return carry
                lax.fori_loop(0, nr, wait_a, 0)

                def send_b(k, carry, q=q):
                    to = lax.rem(r + k, nr)
                    outs[q, to] = mids[q][order[to]]
                    b_copy(q, to, r).start()
                    return carry
                lax.fori_loop(1, nr, send_b, 0)
                rb[2, pl.ds(pl.multiple_of(q * rank + r * sub, sub), sub), :] = mids[q][order[r]]

    for s in (0, 2):
        for q in range(chunks):
            ring_copy(s, q).wait_send()

    for q in range(chunks):
        def done_a(k, carry, q=q):
            a_copy(q, k, 0, q).wait_send()
            return carry
        lax.fori_loop(0, nr, done_a, 0)

        def done_b(k, carry, q=q):
            b_copy(q, lax.rem(r + k, nr), r).wait_send()
            return carry
        lax.fori_loop(1, nr, done_b, 0)


def last_kernel(src_in, rec_in, tile, row_live, col_live, sources, receivers,
                half, half_t, grad, row_mask, rec_new, turned, src_new, sem):
    block, width = tile.shape
    rank = src_in.shape[1]
    chunk = rec_in.shape[1]
    chunks = width // chunk
    step_size = 1.0 / (width + 2 * rank)
    s = row_live.shape[0] - 1
    lanes = row_live[s:s + 1, :].astype(F32)
    rounded_sources(src_in, lanes, half, half_t)
    row_scale(lanes, row_mask, step_size)
    copies = []

    def done(q):
        rows = slice(q * chunk, (q + 1) * chunk)
        turned[rows, :] = rec_new[q * rank:(q + 1) * rank, :].T
        if q % 2 == 1:
            pair = pl.ds((q - 1) * chunk, 2 * chunk)
            copies.append(pltpu.make_async_copy(turned.at[pair], receivers.at[pair], sem.at[q // 2]))
            copies[-1].start()

    sweep(rec_in, rec_new, tile,
          lambda q: col_live[s:s + 1, q * chunk:(q + 1) * chunk].astype(F32),
          half, half_t, grad, step_size, done)
    add_sources(src_new, src_in, row_mask, grad)
    copies.append(pltpu.make_async_copy(src_new, sources, sem.at[chunks // 2]))
    copies[-1].start()
    for copy in copies:
        copy.wait()


def local(nr, nc, tiles, row_live, col_live, row_order, source_init, receiver_init):
    strata, block, width = tiles.shape
    rank = source_init.shape[1]
    chunk = width // CHUNKS
    sub = rank // nr
    vmem = pl.BlockSpec(memory_space=pltpu.VMEM)
    anywhere = pl.BlockSpec(memory_space=pl.ANY)
    sources, receivers, tile = pl.pallas_call(
        functools.partial(main_kernel, nr, nc),
        out_shape=(
            pltpu.VMEM(source_init.shape, F32),
            pltpu.VMEM((CHUNKS * rank, chunk), F32),
            pltpu.VMEM((block, width), BF16),
        ),
        in_specs=[
            anywhere, vmem, vmem, pl.BlockSpec(memory_space=pltpu.SMEM), anywhere, anywhere,
        ],
        out_specs=(vmem, vmem, vmem),
        scratch_shapes=[
            pltpu.VMEM((strata - 1, block, width), BF16),
            pltpu.VMEM((strata, CHUNKS * rank, chunk), F32),
            [pltpu.VMEM((nr, sub, chunk), F32)] * CHUNKS,
            pltpu.VMEM((CHUNKS, nr, sub, chunk), F32),
            pltpu.VMEM(receiver_init.shape, F32),
            pltpu.VMEM((block, rank), F32),
            pltpu.VMEM((block, rank), BF16),
            pltpu.VMEM((rank, block), BF16),
            pltpu.VMEM((block, LANES), F32),
            pltpu.SemaphoreType.DMA((strata + 2,)),
            pltpu.SemaphoreType.DMA((2, CHUNKS)),
            pltpu.SemaphoreType.DMA((2, CHUNKS)),
            pltpu.SemaphoreType.DMA((CHUNKS, nr)),
            pltpu.SemaphoreType.DMA((CHUNKS, nr)),
            pltpu.SemaphoreType.DMA((CHUNKS, nr)),
            pltpu.SemaphoreType.DMA((CHUNKS, nr)),
        ],
        compiler_params=pltpu.CompilerParams(
            collective_id=0, has_side_effects=True, vmem_limit_bytes=56 * 1024 * 1024
        ),
    )(tiles, row_live, col_live, row_order, source_init, receiver_init)
    return pl.pallas_call(
        last_kernel,
        out_shape=(
            jax.ShapeDtypeStruct(source_init.shape, F32),
            jax.ShapeDtypeStruct(receiver_init.shape, F32),
        ),
        in_specs=[vmem] * 5,
        out_specs=(anywhere, anywhere),
        scratch_shapes=[
            pltpu.VMEM((block, rank), BF16),
            pltpu.VMEM((rank, block), BF16),
            pltpu.VMEM((block, rank), F32),
            pltpu.VMEM((block, LANES), F32),
            pltpu.VMEM((CHUNKS * rank, chunk), F32),
            pltpu.VMEM(receiver_init.shape, F32),
            pltpu.VMEM(source_init.shape, F32),
            pltpu.SemaphoreType.DMA((CHUNKS // 2 + 1,)),
        ],
        compiler_params=pltpu.CompilerParams(vmem_limit_bytes=40 * 1024 * 1024),
    )(sources, receivers, tile, row_live, col_live)


def solution(mesh):
    placed = (
        P(None, ("row", "col"), None),
        P(None, ("row", "col")),
        P(None, ("row", "col")),
        P(),
        P(("row", "col"), None),
        P(("row", "col"), None),
    )
    return jax.shard_map(
        functools.partial(local, mesh.shape["row"], mesh.shape["col"]),
        mesh=mesh,
        in_specs=placed,
        out_specs=(P(("row", "col"), None), P(("row", "col"), None)),
        check_vma=False,
    )
```

```python
import functools

import jax
import jax.numpy as jnp
from jax import lax
from jax.experimental import pallas as pl
from jax.experimental.pallas import tpu as pltpu
from jax.sharding import PartitionSpec as P

STEPS = 2
CHUNKS = 4
MESH = pl.DeviceIdType.MESH
F32 = jnp.float32
BF16 = jnp.bfloat16
LANES = 128
LEVELS = 4
PAIR = 2
SUBS = 2
SLOTS = 2
LAG = 2
AHEAD = 3


def rounded_sources(src, lanes, half, half_t):
    half[...] = src[...].astype(BF16)
    half_t[...] = (src[...].T * lanes).astype(BF16)


def row_scale(lanes, row_mask, step_size):
    block = row_mask.shape[0]
    for t in range(block // LANES):
        part = slice(t * LANES, (t + 1) * LANES)
        row_mask[part, :] = jnp.broadcast_to(lanes[:, part], (LANES, LANES)).T * step_size


def misfit_of(half, rec_half, observed):
    predicted = jnp.dot(half[...], rec_half, preferred_element_type=F32)
    return (observed.astype(F32) - predicted).astype(BF16)


def source_gradient(misfit, rec_half, live):
    return lax.dot_general(
        misfit, rec_half * live.astype(BF16), (((1,), (1,)), ((), ())),
        preferred_element_type=F32,
    )


def add_sources(dst, src, row_mask, grad):
    for h in range(src.shape[1] // LANES):
        part = slice(h * LANES, (h + 1) * LANES)
        dst[:, part] = src[:, part] + row_mask[...] * grad[:, part]


def sweep(rec_in, rec_out, observed, live_of, half, half_t, grad, step_size, done=None):
    rank, chunk = half_t.shape[0], rec_in.shape[1]
    chunks = rec_in.shape[0] // rank

    def front(q):
        rec_half = rec_in[q * rank:(q + 1) * rank, :].astype(BF16)
        return rec_half, misfit_of(half, rec_half, observed[:, q * chunk:(q + 1) * chunk])

    ahead = front(0)
    for q in range(chunks):
        rec_half, misfit = ahead
        if q + 1 < chunks:
            ahead = front(q + 1)
        rows = slice(q * rank, (q + 1) * rank)
        live = live_of(q)
        grad_rec = jnp.dot(half_t[...], misfit, preferred_element_type=F32)
        rec_out[rows, :] = rec_in[rows, :] + (step_size * live) * grad_rec
        grad_src = source_gradient(misfit, rec_half, live)
        if q == 0:
            grad[...] = grad_src
        else:
            grad[...] += grad_src
        if done is not None:
            done(q)


class Spread:
    @staticmethod
    def scratch(nr, rank, chunk):
        sub = rank // nr
        return (
            [pltpu.VMEM((nr, sub, chunk), F32)] * CHUNKS,
            pltpu.VMEM((CHUNKS, nr, sub, chunk), F32),
            pltpu.SemaphoreType.DMA((CHUNKS, nr)),
            pltpu.SemaphoreType.DMA((CHUNKS, nr)),
            pltpu.SemaphoreType.DMA((CHUNKS, nr)),
            pltpu.SemaphoreType.DMA((CHUNKS, nr)),
        )

    def __init__(self, nr, nc, rank, chunk, chunks, rb, order, buffers):
        self.nr, self.nc, self.rank, self.chunks, self.rb, self.order = nr, nc, rank, chunks, rb, order
        self.mids, self.outs, self.a_send, self.a_recv, self.b_send, self.b_recv = buffers
        self.r, self.c = lax.axis_index("row"), lax.axis_index("col")
        self.sub = rank // nr

    def rows(self, q, p):
        return pl.ds(q * self.rank + p * self.sub, self.sub)

    def a_copy(self, q, p, slot):
        return pltpu.make_async_remote_copy(
            src_ref=self.rb.at[1, self.rows(q, p)], dst_ref=self.mids[q].at[slot],
            send_sem=self.a_send.at[q, p], recv_sem=self.a_recv.at[q, slot],
            device_id={"row": p, "col": lax.rem(self.c + 1, self.nc)}, device_id_type=MESH,
        )

    def b_copy(self, q, to, p):
        return pltpu.make_async_remote_copy(
            src_ref=self.outs.at[q, to], dst_ref=self.rb.at[2, self.rows(q, p)],
            send_sem=self.b_send.at[q, to], recv_sem=self.b_recv.at[q, p],
            device_id={"row": to, "col": self.c}, device_id_type=MESH,
        )

    def send(self, q):
        slot = lax.rem(self.r + (self.c + 1) // self.nc, self.nr)

        def body(k, carry):
            self.a_copy(q, lax.rem(self.r + k, self.nr), slot).start()
            return carry
        lax.fori_loop(0, self.nr, body, 0)

    def forward(self):
        r, nr = self.r, self.nr
        for q in range(self.chunks):
            def wait_a(k, carry, q=q):
                self.a_copy(q, 0, k).wait_recv()
                return carry
            lax.fori_loop(0, nr, wait_a, 0)

            def send_b(k, carry, q=q):
                to = lax.rem(r + k, nr)
                self.outs[q, to] = self.mids[q][self.order[to]]
                self.b_copy(q, to, r).start()
                return carry
            lax.fori_loop(1, nr, send_b, 0)
            mine = pl.ds(pl.multiple_of(q * self.rank + r * self.sub, self.sub), self.sub)
            self.rb[2, mine, :] = self.mids[q][self.order[r]]

    def arrive(self, q):
        def body(k, carry):
            self.b_copy(q, self.r, lax.rem(self.r + k, self.nr)).wait_recv()
            return carry
        lax.fori_loop(1, self.nr, body, 0)

    def finish(self):
        for q in range(self.chunks):
            def done_a(k, carry, q=q):
                self.a_copy(q, k, 0).wait_send()
                return carry
            lax.fori_loop(0, self.nr, done_a, 0)

            def done_b(k, carry, q=q):
                self.b_copy(q, lax.rem(self.r + k, self.nr), self.r).wait_send()
                return carry
            lax.fori_loop(1, self.nr, done_b, 0)


class Relay:
    @staticmethod
    def scratch(nr, rank, chunk):
        count = CHUNKS * SUBS
        side = nr // 2
        unit = rank // (SUBS * PAIR)
        dma = pltpu.SemaphoreType.DMA
        return (
            [pltpu.VMEM((side, unit, chunk), F32)] * count,
            [pltpu.VMEM((SLOTS, unit, chunk), F32)] * count,
            pltpu.VMEM((count, SLOTS, unit, chunk), F32),
            pltpu.VMEM((count, side, unit, chunk), F32),
            pltpu.VMEM((count, unit, chunk), F32),
            dma((count,)), dma((count,)), dma((count, 2)), dma((count, 3)),
            dma((count,)), dma((count,)), dma((count, side)), dma((count, PAIR)),
        )

    def __init__(self, nr, nc, rank, chunk, chunks, rb, order, buffers):
        (self.pool, self.crossed, self.cross_out, self.deal_out, self.swapped,
         self.x_send, self.x_recv, self.up_send, self.up_recv,
         self.cross_send, self.cross_recv, self.deal_send, self.deal_recv) = buffers
        self.nc, self.rb, self.count = nc, rb, chunks * SUBS
        self.unit = rank // (SUBS * PAIR)
        self.side = side = nr // 2
        self.r, self.c = lax.axis_index("row"), lax.axis_index("col")
        level, self.x = self.r // PAIR, lax.rem(self.r, PAIR)
        upper = self.r // side
        self.base = upper * side
        self.inner = (level == 1) | (level == 2)
        self.hub = (1 + upper) * PAIR
        self.other_hub = (2 - upper) * PAIR
        self.own = self.r - self.base
        self.beside = self.own + 1 - 2 * self.x
        carry = (self.c + 1) // nc

        def source(t):
            row = order[t] - carry
            return jnp.where(row < 0, row + nr, row)

        def inside(row):
            return jnp.where((row >= self.base) & (row < self.base + side), 1, 0)

        self.deals, seen = [], 0
        for j in range(side):
            row = source(self.base + j)
            near = inside(row)
            self.deals.append((near, jnp.where(near == 1, row - self.base, 0),
                               jnp.minimum(jnp.where(near == 1, 0, seen), SLOTS - 1)))
            seen = seen + 1 - near
        self.picks, seen = [0] * SLOTS, 0
        for j in range(side):
            row = source(side - self.base + j)
            near = inside(row)
            for i in range(SLOTS):
                self.picks[i] = jnp.where((near == 1) & (seen == i), row - self.base, self.picks[i])
            seen = seen + near

    def rows(self, m, half):
        return pl.ds(pl.multiple_of((m * PAIR + half) * self.unit, self.unit), self.unit)

    def copy(self, src, dst, send, recv, row, col=None):
        return pltpu.make_async_remote_copy(
            src_ref=src, dst_ref=dst, send_sem=send, recv_sem=recv,
            device_id={"row": row, "col": self.c if col is None else col}, device_id_type=MESH,
        )

    def swap_copy(self, m):
        return self.copy(self.rb.at[1, self.rows(m, 1 - self.x)], self.swapped.at[m],
                         self.x_send.at[m], self.x_recv.at[m], self.base + self.beside)

    def hub_swap_copy(self, m):
        return self.copy(self.rb.at[1, self.rows(m, 1 - self.x)], self.pool[m].at[self.own],
                         self.x_send.at[m], self.up_recv.at[m, 2], self.hub + 1 - self.x)

    def up_copy(self, m):
        return self.copy(self.rb.at[1, self.rows(m, self.x)], self.pool[m].at[self.own],
                         self.up_send.at[m, 0], self.up_recv.at[m, 0], self.hub + self.x)

    def up_beside_copy(self, m):
        return self.copy(self.swapped.at[m], self.pool[m].at[self.beside],
                         self.up_send.at[m, 1], self.up_recv.at[m, 1], self.hub + self.x)

    def cross_copy(self, m):
        return self.copy(self.cross_out.at[m], self.crossed[m],
                         self.cross_send.at[m], self.cross_recv.at[m], self.other_hub + self.x)

    def deal_copy(self, m, j, half):
        return self.copy(self.deal_out.at[m, j], self.rb.at[2, self.rows(m, half)],
                         self.deal_send.at[m, j], self.deal_recv.at[m, half],
                         self.base + j, lax.rem(self.c + 1, self.nc))

    def send(self, q):
        @pl.when(self.inner)
        def _():
            for m in range(q * SUBS, (q + 1) * SUBS):
                self.hub_swap_copy(m).start()
                self.pool[m][self.own] = self.rb[1, self.rows(m, self.x), :]

        @pl.when(jnp.logical_not(self.inner))
        def _():
            for m in range(q * SUBS, (q + 1) * SUBS):
                self.swap_copy(m).start()
                if q == 0:
                    self.up_copy(m).start()

    def gather(self, m):
        for k in range(3):
            self.copy(self.swapped.at[m], self.pool[m].at[0], self.x_send.at[m],
                      self.up_recv.at[m, k], self.r).wait_recv()
        for i in range(SLOTS):
            self.cross_out[m, i] = self.pool[m][self.picks[i]]
        self.cross_copy(m).start()

    def deal(self, m):
        self.cross_copy(m).wait_recv()
        for j in range(self.side):
            near, here, there = self.deals[j]
            self.deal_out[m, j] = jnp.where(near == 1, self.pool[m][here], self.crossed[m][there])
            self.deal_copy(m, j, self.x).start()

    def forward(self):
        @pl.when(jnp.logical_not(self.inner))
        def _():
            for m in range(self.count):
                if m + SUBS < self.count:
                    self.up_copy(m + SUBS).start()
                self.swap_copy(m).wait_recv()
                self.up_beside_copy(m).start()

    def arrive(self, q):
        steps = self.count + LAG
        done = [0] + [min(steps, (k + 1) * SUBS + LAG + AHEAD) for k in range(CHUNKS)]
        for fixed in range(CHUNKS):
            @pl.when((q == fixed) & self.inner)
            def _(fixed=fixed):
                for m in range(done[fixed], steps if fixed + 1 == CHUNKS else done[fixed + 1]):
                    if m < self.count:
                        self.gather(m)
                    if m >= LAG:
                        self.deal(m - LAG)

        def body(i, carry):
            for half in range(PAIR):
                self.deal_copy(q * SUBS + i, 0, half).wait_recv()
            return carry
        lax.fori_loop(0, SUBS, body, 0)

    def finish(self):
        def sent_swap(m, carry):
            self.copy(self.swapped.at[m], self.swapped.at[m], self.x_send.at[m], self.x_recv.at[m], self.r).wait_send()
            return carry
        lax.fori_loop(0, self.count, sent_swap, 0)

        @pl.when(self.inner)
        def _():
            def body(m, carry):
                self.copy(self.cross_out.at[m], self.cross_out.at[m],
                          self.cross_send.at[m], self.cross_recv.at[m], self.r).wait_send()
                for j in range(self.side):
                    self.copy(self.deal_out.at[m, j], self.deal_out.at[m, j],
                              self.deal_send.at[m, j], self.deal_recv.at[m, 0], self.r).wait_send()
                return carry
            lax.fori_loop(0, self.count, body, 0)

        @pl.when(jnp.logical_not(self.inner))
        def _():
            def body(m, carry):
                for k in range(2):
                    self.copy(self.swapped.at[m], self.swapped.at[m],
                              self.up_send.at[m, k], self.up_recv.at[m, 0], self.r).wait_send()
                return carry
            lax.fori_loop(0, self.count, body, 0)


def main_kernel(nr, nc, exchange, tiles, row_live, col_live, order, src_in, rec_in, src_out, rec_out, tile_out,
                tile, rb, stage, grad, half, half_t, row_mask,
                in_sem, ring_send, ring_recv, buffers):
    strata, block, width = tiles.shape
    rank = src_out.shape[1]
    chunk = rb.shape[2]
    chunks = width // chunk
    step_size = 1.0 / (width + 2 * rank)
    r = lax.axis_index("row")
    c = lax.axis_index("col")
    cn = lax.rem(c + 1, nc)
    rn = lax.rem(r + (c + 1) // nc, nr)
    cp = lax.rem(c + nc - 1, nc)

    tile_of = [tile.at[s] for s in range(strata - 1)] + [tile_out]
    loads = [
        pltpu.make_async_copy(rec_in, stage, in_sem.at[strata]),
        pltpu.make_async_copy(src_in, src_out, in_sem.at[strata + 1]),
    ] + [pltpu.make_async_copy(tiles.at[s], tile_of[s], in_sem.at[s]) for s in range(strata)]
    for load in loads:
        load.start()

    barrier = pltpu.get_barrier_semaphore()
    for k in range(nr):
        pl.semaphore_signal(barrier, inc=1, device_id={"row": k, "col": cp}, device_id_type=MESH)
    for k in range(1, nr):
        pl.semaphore_signal(
            barrier, inc=1, device_id={"row": lax.rem(r + k, nr), "col": c}, device_id_type=MESH
        )

    def ring_copy(s, q):
        lane = 0 if s == 0 else 1
        rows = pl.ds(q * rank, rank)
        return pltpu.make_async_remote_copy(
            src_ref=rb.at[s, rows], dst_ref=rb.at[s + 1, rows],
            send_sem=ring_send.at[lane, q], recv_sem=ring_recv.at[lane, q],
            device_id={"row": rn, "col": cn}, device_id_type=MESH,
        )

    moves = exchange(nr, nc, rank, chunk, chunks, rb, order, buffers)

    loads[0].wait()
    for q in range(chunks):
        rb[0, q * rank:(q + 1) * rank, :] = stage[q * chunk:(q + 1) * chunk, :].T
    loads[1].wait()

    for s in range(strata):
        lanes = row_live[s:s + 1, :].astype(F32)
        row_scale(lanes, row_mask, step_size)
        loads[s + 2].wait()
        for it in range(STEPS if s + 1 < strata else STEPS - 1):
            rounded_sources(src_out, lanes, half, half_t)

            def one(q, s=s, it=it):
                rows = pl.ds(pl.multiple_of(q * rank, rank), rank)
                cols = pl.ds(pl.multiple_of(q * chunk, chunk), chunk)
                if it == 0 and s == 2:
                    moves.arrive(q)
                elif it == 0:
                    ring_copy(s - 1, q).wait_recv()
                rec = rb[s, rows, :]
                rec_half = rec.astype(BF16)
                live = col_live[s:s + 1, cols].astype(F32)
                misfit = misfit_of(half, rec_half, tile_of[s][:, cols])
                grad_rec = jnp.dot(half_t[...], misfit, preferred_element_type=F32)
                updated = rec + (step_size * live) * grad_rec
                if s + 1 == strata:
                    rec_out[rows, :] = updated
                else:
                    rb[s, rows, :] = updated
                grad_src = source_gradient(misfit, rec_half, live)

                @pl.when(q == 0)
                def _():
                    grad[...] = grad_src

                @pl.when(q > 0)
                def _():
                    grad[...] += grad_src

                if it == STEPS - 1 and s in (0, 2):
                    ring_copy(s, q).start()
                if it == STEPS - 1 and s == 1:
                    for fixed in range(chunks):
                        pl.when(q == fixed)(functools.partial(moves.send, fixed))

            if it == STEPS - 1 and s == 0:
                pl.semaphore_wait(barrier, 2 * nr - 1)
            if it == 0 and s == 0:
                sweep(rb.at[0], rb.at[0], tile_of[0],
                      lambda q: col_live[0:1, q * chunk:(q + 1) * chunk].astype(F32),
                      half, half_t, grad, step_size)
            else:
                def body(q, carry):
                    one(q)
                    return carry
                lax.fori_loop(0, chunks, body, 0)
            add_sources(src_out, src_out, row_mask, grad)
        if s == 1:
            moves.forward()

    for s in (0, 2):
        for q in range(chunks):
            ring_copy(s, q).wait_send()

    moves.finish()


def last_kernel(src_in, rec_in, tile, row_live, col_live, sources, receivers,
                half, half_t, grad, row_mask, rec_new, turned, src_new, sem):
    block, width = tile.shape
    rank = src_in.shape[1]
    chunk = rec_in.shape[1]
    chunks = width // chunk
    step_size = 1.0 / (width + 2 * rank)
    s = row_live.shape[0] - 1
    lanes = row_live[s:s + 1, :].astype(F32)
    rounded_sources(src_in, lanes, half, half_t)
    row_scale(lanes, row_mask, step_size)
    copies = []

    def done(q):
        rows = slice(q * chunk, (q + 1) * chunk)
        turned[rows, :] = rec_new[q * rank:(q + 1) * rank, :].T
        if q % 2 == 1:
            pair = pl.ds((q - 1) * chunk, 2 * chunk)
            copies.append(pltpu.make_async_copy(turned.at[pair], receivers.at[pair], sem.at[q // 2]))
            copies[-1].start()

    sweep(rec_in, rec_new, tile,
          lambda q: col_live[s:s + 1, q * chunk:(q + 1) * chunk].astype(F32),
          half, half_t, grad, step_size, done)
    add_sources(src_new, src_in, row_mask, grad)
    copies.append(pltpu.make_async_copy(src_new, sources, sem.at[chunks // 2]))
    copies[-1].start()
    for copy in copies:
        copy.wait()


def local(nr, nc, *args):
    if nr != LEVELS * PAIR:
        return run(nr, nc, Spread, 0, *args)
    source = args[3]
    side = nr // 2
    lower = jnp.arange(nr) < side
    near, turned = source < side, (source > 0) & (source <= side)
    weight = (lower & ~near).astype(jnp.int32) + nr * (lower & ~turned).astype(jnp.int32)
    crossing = jnp.sum(weight)
    return lax.cond(
        jnp.maximum(crossing % nr, crossing // nr) <= SLOTS,
        functools.partial(run, nr, nc, Relay, 1),
        functools.partial(run, nr, nc, Spread, 0),
        *args,
    )


def run(nr, nc, exchange, collective_id, tiles, row_live, col_live, row_order, source_init, receiver_init):
    strata, block, width = tiles.shape
    rank = source_init.shape[1]
    chunk = width // CHUNKS
    vmem = pl.BlockSpec(memory_space=pltpu.VMEM)
    anywhere = pl.BlockSpec(memory_space=pl.ANY)
    sources, receivers, tile = pl.pallas_call(
        functools.partial(main_kernel, nr, nc, exchange),
        out_shape=(
            pltpu.VMEM(source_init.shape, F32),
            pltpu.VMEM((CHUNKS * rank, chunk), F32),
            pltpu.VMEM((block, width), BF16),
        ),
        in_specs=[
            anywhere, vmem, vmem, pl.BlockSpec(memory_space=pltpu.SMEM), anywhere, anywhere,
        ],
        out_specs=(vmem, vmem, vmem),
        scratch_shapes=[
            pltpu.VMEM((strata - 1, block, width), BF16),
            pltpu.VMEM((strata, CHUNKS * rank, chunk), F32),
            pltpu.VMEM(receiver_init.shape, F32),
            pltpu.VMEM((block, rank), F32),
            pltpu.VMEM((block, rank), BF16),
            pltpu.VMEM((rank, block), BF16),
            pltpu.VMEM((block, LANES), F32),
            pltpu.SemaphoreType.DMA((strata + 2,)),
            pltpu.SemaphoreType.DMA((2, CHUNKS)),
            pltpu.SemaphoreType.DMA((2, CHUNKS)),
            exchange.scratch(nr, rank, chunk),
        ],
        compiler_params=pltpu.CompilerParams(
            collective_id=collective_id, has_side_effects=True, vmem_limit_bytes=56 * 1024 * 1024
        ),
    )(tiles, row_live, col_live, row_order, source_init, receiver_init)
    return pl.pallas_call(
        last_kernel,
        out_shape=(
            jax.ShapeDtypeStruct(source_init.shape, F32),
            jax.ShapeDtypeStruct(receiver_init.shape, F32),
        ),
        in_specs=[vmem] * 5,
        out_specs=(anywhere, anywhere),
        scratch_shapes=[
            pltpu.VMEM((block, rank), BF16),
            pltpu.VMEM((rank, block), BF16),
            pltpu.VMEM((block, rank), F32),
            pltpu.VMEM((block, LANES), F32),
            pltpu.VMEM((CHUNKS * rank, chunk), F32),
            pltpu.VMEM(receiver_init.shape, F32),
            pltpu.VMEM(source_init.shape, F32),
            pltpu.SemaphoreType.DMA((CHUNKS // 2 + 1,)),
        ],
        compiler_params=pltpu.CompilerParams(vmem_limit_bytes=40 * 1024 * 1024),
    )(sources, receivers, tile, row_live, col_live)


def solution(mesh):
    placed = (
        P(None, ("row", "col"), None),
        P(None, ("row", "col")),
        P(None, ("row", "col")),
        P(),
        P(("row", "col"), None),
        P(("row", "col"), None),
    )
    return jax.shard_map(
        functools.partial(local, mesh.shape["row"], mesh.shape["col"]),
        mesh=mesh,
        in_specs=placed,
        out_specs=(P(("row", "col"), None), P(("row", "col"), None)),
        check_vma=False,
    )
```

```python
import functools

import jax
import jax.numpy as jnp
from jax import lax
from jax.experimental import pallas as pl
from jax.experimental.pallas import tpu as pltpu
from jax.sharding import PartitionSpec as P

STEPS = 2
CHUNKS = 4
MESH = pl.DeviceIdType.MESH
F32 = jnp.float32
BF16 = jnp.bfloat16
LANES = 128
LEVELS = 4
PAIR = 2
SUBS = 2
SLOTS = 2
LAG = 2
AHEAD = 3
DIRECT = 2
EARLY = 1


def rounded_sources(src, lanes, half, half_t):
    half[...] = src[...].astype(BF16)
    half_t[...] = (src[...].T * lanes).astype(BF16)


def row_scale(lanes, row_mask, step_size):
    block = row_mask.shape[0]
    for t in range(block // LANES):
        part = slice(t * LANES, (t + 1) * LANES)
        row_mask[part, :] = jnp.broadcast_to(lanes[:, part], (LANES, LANES)).T * step_size


def misfit_of(half, rec_half, observed):
    predicted = jnp.dot(half[...], rec_half, preferred_element_type=F32)
    return (observed.astype(F32) - predicted).astype(BF16)


def source_gradient(misfit, rec_half, live):
    return lax.dot_general(
        misfit, rec_half * live.astype(BF16), (((1,), (1,)), ((), ())),
        preferred_element_type=F32,
    )


def add_sources(dst, src, row_mask, grad):
    for h in range(src.shape[1] // LANES):
        part = slice(h * LANES, (h + 1) * LANES)
        dst[:, part] = src[:, part] + row_mask[...] * grad[:, part]


def sweep(rec_in, rec_out, observed, live_of, half, half_t, grad, step_size, done=None):
    rank, chunk = half_t.shape[0], rec_in.shape[1]
    chunks = rec_in.shape[0] // rank

    def front(q):
        rec_half = rec_in[q * rank:(q + 1) * rank, :].astype(BF16)
        return rec_half, misfit_of(half, rec_half, observed[:, q * chunk:(q + 1) * chunk])

    ahead = front(0)
    for q in range(chunks):
        rec_half, misfit = ahead
        if q + 1 < chunks:
            ahead = front(q + 1)
        rows = slice(q * rank, (q + 1) * rank)
        live = live_of(q)
        grad_rec = jnp.dot(half_t[...], misfit, preferred_element_type=F32)
        rec_out[rows, :] = rec_in[rows, :] + (step_size * live) * grad_rec
        grad_src = source_gradient(misfit, rec_half, live)
        if q == 0:
            grad[...] = grad_src
        else:
            grad[...] += grad_src
        if done is not None:
            done(q)


class Spread:
    @staticmethod
    def scratch(nr, rank, chunk):
        sub = rank // nr
        return (
            [pltpu.VMEM((nr, sub, chunk), F32)] * CHUNKS,
            pltpu.VMEM((CHUNKS, nr, sub, chunk), F32),
            pltpu.SemaphoreType.DMA((CHUNKS, nr)),
            pltpu.SemaphoreType.DMA((CHUNKS, nr)),
            pltpu.SemaphoreType.DMA((CHUNKS, nr)),
            pltpu.SemaphoreType.DMA((CHUNKS, nr)),
        )

    def __init__(self, nr, nc, rank, chunk, chunks, rb, order, buffers):
        self.nr, self.nc, self.rank, self.chunks, self.rb, self.order = nr, nc, rank, chunks, rb, order
        self.mids, self.outs, self.a_send, self.a_recv, self.b_send, self.b_recv = buffers
        self.r, self.c = lax.axis_index("row"), lax.axis_index("col")
        self.sub = rank // nr

    def rows(self, q, p):
        return pl.ds(q * self.rank + p * self.sub, self.sub)

    def a_copy(self, q, p, slot):
        return pltpu.make_async_remote_copy(
            src_ref=self.rb.at[1, self.rows(q, p)], dst_ref=self.mids[q].at[slot],
            send_sem=self.a_send.at[q, p], recv_sem=self.a_recv.at[q, slot],
            device_id={"row": p, "col": lax.rem(self.c + 1, self.nc)}, device_id_type=MESH,
        )

    def b_copy(self, q, to, p):
        return pltpu.make_async_remote_copy(
            src_ref=self.outs.at[q, to], dst_ref=self.rb.at[2, self.rows(q, p)],
            send_sem=self.b_send.at[q, to], recv_sem=self.b_recv.at[q, p],
            device_id={"row": to, "col": self.c}, device_id_type=MESH,
        )

    def send(self, q):
        slot = lax.rem(self.r + (self.c + 1) // self.nc, self.nr)

        def body(k, carry):
            self.a_copy(q, lax.rem(self.r + k, self.nr), slot).start()
            return carry
        lax.fori_loop(0, self.nr, body, 0)

    def forward(self):
        r, nr = self.r, self.nr
        for q in range(self.chunks):
            def wait_a(k, carry, q=q):
                self.a_copy(q, 0, k).wait_recv()
                return carry
            lax.fori_loop(0, nr, wait_a, 0)

            def send_b(k, carry, q=q):
                to = lax.rem(r + k, nr)
                self.outs[q, to] = self.mids[q][self.order[to]]
                self.b_copy(q, to, r).start()
                return carry
            lax.fori_loop(1, nr, send_b, 0)
            mine = pl.ds(pl.multiple_of(q * self.rank + r * self.sub, self.sub), self.sub)
            self.rb[2, mine, :] = self.mids[q][self.order[r]]

    def arrive(self, q):
        def body(k, carry):
            self.b_copy(q, self.r, lax.rem(self.r + k, self.nr)).wait_recv()
            return carry
        lax.fori_loop(1, self.nr, body, 0)

    def finish(self):
        for q in range(self.chunks):
            def done_a(k, carry, q=q):
                self.a_copy(q, k, 0).wait_send()
                return carry
            lax.fori_loop(0, self.nr, done_a, 0)

            def done_b(k, carry, q=q):
                self.b_copy(q, lax.rem(self.r + k, self.nr), self.r).wait_send()
                return carry
            lax.fori_loop(1, self.nr, done_b, 0)


class Relay:
    @staticmethod
    def scratch(nr, rank, chunk):
        count = CHUNKS * SUBS
        side = nr // 2
        unit = rank // (SUBS * PAIR)
        dma = pltpu.SemaphoreType.DMA
        return (
            [pltpu.VMEM((side, unit, chunk), F32)] * count,
            [pltpu.VMEM((SLOTS, unit, chunk), F32)] * count,
            pltpu.VMEM((count, SLOTS, unit, chunk), F32),
            pltpu.VMEM((count, side, unit, chunk), F32),
            pltpu.VMEM((count, unit, chunk), F32),
            dma((count,)), dma((count,)), dma((count, 2)), dma((count, 3)),
            dma((count,)), dma((count,)), dma((count, side)), dma((count, PAIR)),
        )

    def __init__(self, nr, nc, rank, chunk, chunks, rb, order, buffers):
        (self.pool, self.crossed, self.cross_out, self.deal_out, self.swapped,
         self.x_send, self.x_recv, self.up_send, self.up_recv,
         self.cross_send, self.cross_recv, self.deal_send, self.deal_recv) = buffers
        self.nc, self.rb, self.count = nc, rb, chunks * SUBS
        self.unit = rank // (SUBS * PAIR)
        self.side = side = nr // 2
        self.r, self.c = lax.axis_index("row"), lax.axis_index("col")
        level, self.x = self.r // PAIR, lax.rem(self.r, PAIR)
        upper = self.r // side
        self.base = upper * side
        self.inner = (level == 1) | (level == 2)
        self.hub = (1 + upper) * PAIR
        self.other_hub = (2 - upper) * PAIR
        self.own = self.r - self.base
        self.beside = self.own + 1 - 2 * self.x
        carry = (self.c + 1) // nc

        def source(t):
            row = order[t] - carry
            return jnp.where(row < 0, row + nr, row)

        def inside(row):
            return jnp.where((row >= self.base) & (row < self.base + side), 1, 0)

        self.deals, seen = [], 0
        for j in range(side):
            row = source(self.base + j)
            near = inside(row)
            self.deals.append((near, jnp.where(near == 1, row - self.base, 0),
                               jnp.minimum(jnp.where(near == 1, 0, seen), SLOTS - 1)))
            seen = seen + 1 - near
        self.picks, seen = [0] * SLOTS, 0
        for j in range(side):
            row = source(side - self.base + j)
            near = inside(row)
            for i in range(SLOTS):
                self.picks[i] = jnp.where((near == 1) & (seen == i), row - self.base, self.picks[i])
            seen = seen + near

    def rows(self, m, half):
        return pl.ds(pl.multiple_of((m * PAIR + half) * self.unit, self.unit), self.unit)

    def copy(self, src, dst, send, recv, row, col=None):
        return pltpu.make_async_remote_copy(
            src_ref=src, dst_ref=dst, send_sem=send, recv_sem=recv,
            device_id={"row": row, "col": self.c if col is None else col}, device_id_type=MESH,
        )

    def swap_copy(self, m):
        return self.copy(self.rb.at[1, self.rows(m, 1 - self.x)], self.swapped.at[m],
                         self.x_send.at[m], self.x_recv.at[m], self.base + self.beside)

    def hub_swap_copy(self, m):
        return self.copy(self.rb.at[1, self.rows(m, 1 - self.x)], self.pool[m].at[self.own],
                         self.x_send.at[m], self.up_recv.at[m, 2], self.hub + 1 - self.x)

    def up_copy(self, m):
        return self.copy(self.rb.at[1, self.rows(m, self.x)], self.pool[m].at[self.own],
                         self.up_send.at[m, 0], self.up_recv.at[m, 0], self.hub + self.x)

    def diagonal_copy(self, m):
        return self.copy(self.rb.at[1, self.rows(m, 1 - self.x)], self.pool[m].at[self.own],
                         self.up_send.at[m, 1], self.up_recv.at[m, 1], self.hub + 1 - self.x)

    def up_beside_copy(self, m):
        return self.copy(self.swapped.at[m], self.pool[m].at[self.beside],
                         self.up_send.at[m, 1], self.up_recv.at[m, 1], self.hub + self.x)

    def cross_copy(self, m):
        return self.copy(self.cross_out.at[m], self.crossed[m],
                         self.cross_send.at[m], self.cross_recv.at[m], self.other_hub + self.x)

    def deal_copy(self, m, j, half):
        return self.copy(self.deal_out.at[m, j], self.rb.at[2, self.rows(m, half)],
                         self.deal_send.at[m, j], self.deal_recv.at[m, half],
                         self.base + j, lax.rem(self.c + 1, self.nc))

    def send(self, q):
        @pl.when(self.inner)
        def _():
            for m in range(q * SUBS, (q + 1) * SUBS):
                self.hub_swap_copy(m).start()
                self.pool[m][self.own] = self.rb[1, self.rows(m, self.x), :]

        @pl.when(jnp.logical_not(self.inner))
        def _():
            for m in range(q * SUBS, (q + 1) * SUBS):
                if m < DIRECT:
                    self.up_copy(m).start()
                    self.diagonal_copy(m).start()
                else:
                    self.swap_copy(m).start()

    def gather(self, m):
        for k in range(3):
            self.copy(self.swapped.at[m], self.pool[m].at[0], self.x_send.at[m],
                      self.up_recv.at[m, k], self.r).wait_recv()
        for i in range(SLOTS):
            self.cross_out[m, i] = self.pool[m][self.picks[i]]
        self.cross_copy(m).start()

    def deal(self, m):
        self.cross_copy(m).wait_recv()
        for j in range(self.side):
            near, here, there = self.deals[j]
            self.deal_out[m, j] = jnp.where(near == 1, self.pool[m][here], self.crossed[m][there])
            self.deal_copy(m, j, self.x).start()

    def forward(self):
        @pl.when(jnp.logical_not(self.inner))
        def _():
            for m in range(DIRECT, self.count):
                self.up_copy(m).start()
                self.swap_copy(m).wait_recv()
                self.up_beside_copy(m).start()

        @pl.when(self.inner)
        def _():
            for m in range(EARLY):
                self.gather(m)

    def arrive(self, q):
        steps = self.count + LAG
        done = [0] + [min(steps, (k + 1) * SUBS + LAG + AHEAD) for k in range(CHUNKS)]
        for fixed in range(CHUNKS):
            @pl.when((q == fixed) & self.inner)
            def _(fixed=fixed):
                for m in range(done[fixed], steps if fixed + 1 == CHUNKS else done[fixed + 1]):
                    if EARLY <= m < self.count:
                        self.gather(m)
                    if m >= LAG:
                        self.deal(m - LAG)

        def body(i, carry):
            for half in range(PAIR):
                self.deal_copy(q * SUBS + i, 0, half).wait_recv()
            return carry
        lax.fori_loop(0, SUBS, body, 0)

    def finish(self):
        def sent_swap(m, carry):
            self.copy(self.swapped.at[m], self.swapped.at[m], self.x_send.at[m], self.x_recv.at[m], self.r).wait_send()
            return carry
        @pl.when(self.inner)
        def _():
            lax.fori_loop(0, self.count, sent_swap, 0)

            def body(m, carry):
                self.copy(self.cross_out.at[m], self.cross_out.at[m],
                          self.cross_send.at[m], self.cross_recv.at[m], self.r).wait_send()
                for j in range(self.side):
                    self.copy(self.deal_out.at[m, j], self.deal_out.at[m, j],
                              self.deal_send.at[m, j], self.deal_recv.at[m, 0], self.r).wait_send()
                return carry
            lax.fori_loop(0, self.count, body, 0)

        @pl.when(jnp.logical_not(self.inner))
        def _():
            lax.fori_loop(DIRECT, self.count, sent_swap, 0)

            def body(m, carry):
                for k in range(2):
                    self.copy(self.swapped.at[m], self.swapped.at[m],
                              self.up_send.at[m, k], self.up_recv.at[m, 0], self.r).wait_send()
                return carry
            lax.fori_loop(0, self.count, body, 0)


def main_kernel(nr, nc, exchange, tiles, row_live, col_live, order, src_in, rec_in, src_out, rec_out, tile_out,
                tile, rb, stage, grad, half, half_t, row_mask,
                in_sem, ring_send, ring_recv, buffers):
    strata, block, width = tiles.shape
    rank = src_out.shape[1]
    chunk = rb.shape[2]
    chunks = width // chunk
    step_size = 1.0 / (width + 2 * rank)
    r = lax.axis_index("row")
    c = lax.axis_index("col")
    cn = lax.rem(c + 1, nc)
    rn = lax.rem(r + (c + 1) // nc, nr)
    cp = lax.rem(c + nc - 1, nc)

    tile_of = [tile.at[s] for s in range(strata - 1)] + [tile_out]
    loads = [
        pltpu.make_async_copy(rec_in, stage, in_sem.at[strata]),
        pltpu.make_async_copy(src_in, src_out, in_sem.at[strata + 1]),
    ] + [pltpu.make_async_copy(tiles.at[s], tile_of[s], in_sem.at[s]) for s in range(strata)]
    for load in loads[:3]:
        load.start()

    barrier = pltpu.get_barrier_semaphore()
    for k in range(nr):
        pl.semaphore_signal(barrier, inc=1, device_id={"row": k, "col": cp}, device_id_type=MESH)
    for k in range(1, nr):
        pl.semaphore_signal(
            barrier, inc=1, device_id={"row": lax.rem(r + k, nr), "col": c}, device_id_type=MESH
        )

    def ring_copy(s, q):
        lane = 0 if s == 0 else 1
        rows = pl.ds(q * rank, rank)
        return pltpu.make_async_remote_copy(
            src_ref=rb.at[s, rows], dst_ref=rb.at[s + 1, rows],
            send_sem=ring_send.at[lane, q], recv_sem=ring_recv.at[lane, q],
            device_id={"row": rn, "col": cn}, device_id_type=MESH,
        )

    moves = exchange(nr, nc, rank, chunk, chunks, rb, order, buffers)

    loads[0].wait()
    for q in range(chunks):
        rb[0, q * rank:(q + 1) * rank, :] = stage[q * chunk:(q + 1) * chunk, :].T
    loads[1].wait()

    for s in range(strata):
        lanes = row_live[s:s + 1, :].astype(F32)
        row_scale(lanes, row_mask, step_size)
        loads[s + 2].wait()
        if s == 0:
            for load in loads[3:]:
                load.start()
        for it in range(STEPS if s + 1 < strata else STEPS - 1):
            rounded_sources(src_out, lanes, half, half_t)

            def one(q, s=s, it=it):
                rows = pl.ds(pl.multiple_of(q * rank, rank), rank)
                cols = pl.ds(pl.multiple_of(q * chunk, chunk), chunk)
                if it == 0 and s == 2:
                    moves.arrive(q)
                elif it == 0:
                    ring_copy(s - 1, q).wait_recv()
                rec = rb[s, rows, :]
                rec_half = rec.astype(BF16)
                live = col_live[s:s + 1, cols].astype(F32)
                misfit = misfit_of(half, rec_half, tile_of[s][:, cols])
                grad_rec = jnp.dot(half_t[...], misfit, preferred_element_type=F32)
                updated = rec + (step_size * live) * grad_rec
                if s + 1 == strata:
                    rec_out[rows, :] = updated
                else:
                    rb[s, rows, :] = updated
                if it == STEPS - 1 and s in (0, 2):
                    ring_copy(s, q).start()
                if it == STEPS - 1 and s == 1:
                    for fixed in range(chunks):
                        pl.when(q == fixed)(functools.partial(moves.send, fixed))
                grad_src = source_gradient(misfit, rec_half, live)

                @pl.when(q == 0)
                def _():
                    grad[...] = grad_src

                @pl.when(q > 0)
                def _():
                    grad[...] += grad_src

            if it == STEPS - 1 and s == 0:
                pl.semaphore_wait(barrier, 2 * nr - 1)
            if it == 0 and s == 0:
                sweep(rb.at[0], rb.at[0], tile_of[0],
                      lambda q: col_live[0:1, q * chunk:(q + 1) * chunk].astype(F32),
                      half, half_t, grad, step_size)
            else:
                def body(q, carry):
                    one(q)
                    return carry
                lax.fori_loop(0, chunks, body, 0)
            if it == STEPS - 1 and s == 1:
                moves.forward()
            add_sources(src_out, src_out, row_mask, grad)
    for s in (0, 2):
        for q in range(chunks):
            ring_copy(s, q).wait_send()

    moves.finish()


def last_kernel(src_in, rec_in, tile, row_live, col_live, sources, receivers,
                half, half_t, grad, row_mask, rec_new, turned, src_new, sem):
    block, width = tile.shape
    rank = src_in.shape[1]
    chunk = rec_in.shape[1]
    chunks = width // chunk
    step_size = 1.0 / (width + 2 * rank)
    s = row_live.shape[0] - 1
    lanes = row_live[s:s + 1, :].astype(F32)
    rounded_sources(src_in, lanes, half, half_t)
    row_scale(lanes, row_mask, step_size)
    copies = []

    def done(q):
        rows = slice(q * chunk, (q + 1) * chunk)
        turned[rows, :] = rec_new[q * rank:(q + 1) * rank, :].T
        if q % 2 == 1:
            pair = pl.ds((q - 1) * chunk, 2 * chunk)
            copies.append(pltpu.make_async_copy(turned.at[pair], receivers.at[pair], sem.at[q // 2]))
            copies[-1].start()

    sweep(rec_in, rec_new, tile,
          lambda q: col_live[s:s + 1, q * chunk:(q + 1) * chunk].astype(F32),
          half, half_t, grad, step_size, done)
    add_sources(src_new, src_in, row_mask, grad)
    copies.append(pltpu.make_async_copy(src_new, sources, sem.at[chunks // 2]))
    copies[-1].start()
    for copy in copies:
        copy.wait()


def local(nr, nc, *args):
    if nr != LEVELS * PAIR:
        return run(nr, nc, Spread, 0, *args)
    source = args[3]
    side = nr // 2
    lower = jnp.arange(nr) < side
    direct = (lower & (source >= side)).astype(jnp.int32)
    shifted = (lower & ((source > side) | (source == 0))).astype(jnp.int32)
    field = 2 * nr
    spare = nr - SLOTS - 1
    crossing = jnp.sum(direct + field * shifted) + spare * (1 + field)
    return lax.cond(
        (crossing & (nr * (1 + field))) == 0,
        functools.partial(run, nr, nc, Relay, 1),
        functools.partial(run, nr, nc, Spread, 0),
        *args,
    )


def run(nr, nc, exchange, collective_id, tiles, row_live, col_live, row_order, source_init, receiver_init):
    strata, block, width = tiles.shape
    rank = source_init.shape[1]
    chunk = width // CHUNKS
    vmem = pl.BlockSpec(memory_space=pltpu.VMEM)
    anywhere = pl.BlockSpec(memory_space=pl.ANY)
    sources, receivers, tile = pl.pallas_call(
        functools.partial(main_kernel, nr, nc, exchange),
        out_shape=(
            pltpu.VMEM(source_init.shape, F32),
            pltpu.VMEM((CHUNKS * rank, chunk), F32),
            pltpu.VMEM((block, width), BF16),
        ),
        in_specs=[
            anywhere, vmem, vmem, pl.BlockSpec(memory_space=pltpu.SMEM), anywhere, anywhere,
        ],
        out_specs=(vmem, vmem, vmem),
        scratch_shapes=[
            pltpu.VMEM((strata - 1, block, width), BF16),
            pltpu.VMEM((strata, CHUNKS * rank, chunk), F32),
            pltpu.VMEM(receiver_init.shape, F32),
            pltpu.VMEM((block, rank), F32),
            pltpu.VMEM((block, rank), BF16),
            pltpu.VMEM((rank, block), BF16),
            pltpu.VMEM((block, LANES), F32),
            pltpu.SemaphoreType.DMA((strata + 2,)),
            pltpu.SemaphoreType.DMA((2, CHUNKS)),
            pltpu.SemaphoreType.DMA((2, CHUNKS)),
            exchange.scratch(nr, rank, chunk),
        ],
        compiler_params=pltpu.CompilerParams(
            collective_id=collective_id, has_side_effects=True, vmem_limit_bytes=56 * 1024 * 1024
        ),
    )(tiles, row_live, col_live, row_order, source_init, receiver_init)
    return pl.pallas_call(
        last_kernel,
        out_shape=(
            jax.ShapeDtypeStruct(source_init.shape, F32),
            jax.ShapeDtypeStruct(receiver_init.shape, F32),
        ),
        in_specs=[vmem] * 5,
        out_specs=(anywhere, anywhere),
        scratch_shapes=[
            pltpu.VMEM((block, rank), BF16),
            pltpu.VMEM((rank, block), BF16),
            pltpu.VMEM((block, rank), F32),
            pltpu.VMEM((block, LANES), F32),
            pltpu.VMEM((CHUNKS * rank, chunk), F32),
            pltpu.VMEM(receiver_init.shape, F32),
            pltpu.VMEM(source_init.shape, F32),
            pltpu.SemaphoreType.DMA((CHUNKS // 2 + 1,)),
        ],
        compiler_params=pltpu.CompilerParams(vmem_limit_bytes=40 * 1024 * 1024),
    )(sources, receivers, tile, row_live, col_live)


def solution(mesh):
    placed = (
        P(None, ("row", "col"), None),
        P(None, ("row", "col")),
        P(None, ("row", "col")),
        P(),
        P(("row", "col"), None),
        P(("row", "col"), None),
    )
    return jax.shard_map(
        functools.partial(local, mesh.shape["row"], mesh.shape["col"]),
        mesh=mesh,
        in_specs=placed,
        out_specs=(P(("row", "col"), None), P(("row", "col"), None)),
        check_vma=False,
    )
```

```python
import functools

import jax
import jax.numpy as jnp
from jax import lax
from jax.experimental import pallas as pl
from jax.experimental.pallas import tpu as pltpu
from jax.sharding import PartitionSpec as P

STEPS = 2
CHUNKS = 4
MESH = pl.DeviceIdType.MESH
F32 = jnp.float32
BF16 = jnp.bfloat16
LANES = 128
LEVELS = 4
PAIR = 2
SUBS = 2
LAG = 2
AHEAD = 3
DIRECT = 2
EARLY = 1


def rounded_sources(src, lanes, half, half_t):
    half[...] = src[...].astype(BF16)
    half_t[...] = (src[...].T * lanes).astype(BF16)


def row_scale(lanes, row_mask, step_size):
    block = row_mask.shape[0]
    for t in range(block // LANES):
        part = slice(t * LANES, (t + 1) * LANES)
        row_mask[part, :] = jnp.broadcast_to(lanes[:, part], (LANES, LANES)).T * step_size


def misfit_of(half, rec_half, observed):
    predicted = jnp.dot(half[...], rec_half, preferred_element_type=F32)
    return (observed.astype(F32) - predicted).astype(BF16)


def source_gradient(misfit, rec_half, live):
    return lax.dot_general(
        misfit, rec_half * live.astype(BF16), (((1,), (1,)), ((), ())),
        preferred_element_type=F32,
    )


def add_sources(dst, src, row_mask, grad):
    for h in range(src.shape[1] // LANES):
        part = slice(h * LANES, (h + 1) * LANES)
        dst[:, part] = src[:, part] + row_mask[...] * grad[:, part]


def sweep(rec_in, rec_out, observed, live_of, half, half_t, grad, step_size, done=None):
    rank, chunk = half_t.shape[0], rec_in.shape[1]
    chunks = rec_in.shape[0] // rank

    def front(q):
        rec_half = rec_in[q * rank:(q + 1) * rank, :].astype(BF16)
        return rec_half, misfit_of(half, rec_half, observed[:, q * chunk:(q + 1) * chunk])

    ahead = front(0)
    for q in range(chunks):
        rec_half, misfit = ahead
        if q + 1 < chunks:
            ahead = front(q + 1)
        rows = slice(q * rank, (q + 1) * rank)
        live = live_of(q)
        grad_rec = jnp.dot(half_t[...], misfit, preferred_element_type=F32)
        rec_out[rows, :] = rec_in[rows, :] + (step_size * live) * grad_rec
        grad_src = source_gradient(misfit, rec_half, live)
        if q == 0:
            grad[...] = grad_src
        else:
            grad[...] += grad_src
        if done is not None:
            done(q)


class Spread:
    @staticmethod
    def scratch(nr, rank, chunk):
        sub = rank // nr
        return (
            [pltpu.VMEM((nr, sub, chunk), F32)] * CHUNKS,
            pltpu.VMEM((CHUNKS, nr, sub, chunk), F32),
            pltpu.SemaphoreType.DMA((CHUNKS, nr)),
            pltpu.SemaphoreType.DMA((CHUNKS, nr)),
            pltpu.SemaphoreType.DMA((CHUNKS, nr)),
            pltpu.SemaphoreType.DMA((CHUNKS, nr)),
        )

    def __init__(self, nr, nc, rank, chunk, chunks, rb, order, buffers):
        self.nr, self.nc, self.rank, self.chunks, self.rb, self.order = nr, nc, rank, chunks, rb, order
        self.mids, self.outs, self.a_send, self.a_recv, self.b_send, self.b_recv = buffers
        self.r, self.c = lax.axis_index("row"), lax.axis_index("col")
        self.sub = rank // nr

    def rows(self, q, p):
        return pl.ds(q * self.rank + p * self.sub, self.sub)

    def a_copy(self, q, p, slot):
        return pltpu.make_async_remote_copy(
            src_ref=self.rb.at[1, self.rows(q, p)], dst_ref=self.mids[q].at[slot],
            send_sem=self.a_send.at[q, p], recv_sem=self.a_recv.at[q, slot],
            device_id={"row": p, "col": lax.rem(self.c + 1, self.nc)}, device_id_type=MESH,
        )

    def b_copy(self, q, to, p):
        return pltpu.make_async_remote_copy(
            src_ref=self.outs.at[q, to], dst_ref=self.rb.at[2, self.rows(q, p)],
            send_sem=self.b_send.at[q, to], recv_sem=self.b_recv.at[q, p],
            device_id={"row": to, "col": self.c}, device_id_type=MESH,
        )

    def send(self, q):
        slot = lax.rem(self.r + (self.c + 1) // self.nc, self.nr)

        def body(k, carry):
            self.a_copy(q, lax.rem(self.r + k, self.nr), slot).start()
            return carry
        lax.fori_loop(0, self.nr, body, 0)

    def forward(self):
        r, nr = self.r, self.nr
        for q in range(self.chunks):
            def wait_a(k, carry, q=q):
                self.a_copy(q, 0, k).wait_recv()
                return carry
            lax.fori_loop(0, nr, wait_a, 0)

            def send_b(k, carry, q=q):
                to = lax.rem(r + k, nr)
                self.outs[q, to] = self.mids[q][self.order[to]]
                self.b_copy(q, to, r).start()
                return carry
            lax.fori_loop(1, nr, send_b, 0)
            mine = pl.ds(pl.multiple_of(q * self.rank + r * self.sub, self.sub), self.sub)
            self.rb[2, mine, :] = self.mids[q][self.order[r]]

    def arrive(self, q):
        def body(k, carry):
            self.b_copy(q, self.r, lax.rem(self.r + k, self.nr)).wait_recv()
            return carry
        lax.fori_loop(1, self.nr, body, 0)

    def finish(self):
        for q in range(self.chunks):
            def done_a(k, carry, q=q):
                self.a_copy(q, k, 0).wait_send()
                return carry
            lax.fori_loop(0, self.nr, done_a, 0)

            def done_b(k, carry, q=q):
                self.b_copy(q, lax.rem(self.r + k, self.nr), self.r).wait_send()
                return carry
            lax.fori_loop(1, self.nr, done_b, 0)


class Relay:
    def __init__(self, slots):
        self.slots = slots

    def scratch(self, nr, rank, chunk):
        count = CHUNKS * SUBS
        side = nr // 2
        unit = rank // (SUBS * PAIR)
        dma = pltpu.SemaphoreType.DMA
        return (
            [pltpu.VMEM((side, unit, chunk), F32)] * count,
            [pltpu.VMEM((self.slots, unit, chunk), F32)] * count,
            pltpu.VMEM((count, self.slots, unit, chunk), F32),
            pltpu.VMEM((count, side, unit, chunk), F32),
            pltpu.VMEM((count, unit, chunk), F32),
            dma((count,)), dma((count,)), dma((count, 2)), dma((count, 3)),
            dma((count,)), dma((count,)), dma((count, side)), dma((count, PAIR)),
        )

    def __call__(self, nr, nc, rank, chunk, chunks, rb, order, buffers):
        (self.pool, self.crossed, self.cross_out, self.deal_out, self.swapped,
         self.x_send, self.x_recv, self.up_send, self.up_recv,
         self.cross_send, self.cross_recv, self.deal_send, self.deal_recv) = buffers
        self.nc, self.rb, self.count = nc, rb, chunks * SUBS
        self.unit = rank // (SUBS * PAIR)
        self.side = side = nr // 2
        self.r, self.c = lax.axis_index("row"), lax.axis_index("col")
        level, self.x = self.r // PAIR, lax.rem(self.r, PAIR)
        upper = self.r // side
        self.base = upper * side
        self.inner = (level == 1) | (level == 2)
        self.hub = (1 + upper) * PAIR
        self.other_hub = (2 - upper) * PAIR
        self.own = self.r - self.base
        self.beside = self.own + 1 - 2 * self.x
        carry = (self.c + 1) // nc

        def source(t):
            row = order[t] - carry
            return jnp.where(row < 0, row + nr, row)

        def inside(row):
            return jnp.where((row >= self.base) & (row < self.base + side), 1, 0)

        self.deals, seen = [], 0
        for j in range(side):
            row = source(self.base + j)
            near = inside(row)
            self.deals.append((near, jnp.where(near == 1, row - self.base, 0),
                               jnp.minimum(jnp.where(near == 1, 0, seen), self.slots - 1)))
            seen = seen + 1 - near
        self.picks, seen = [0] * self.slots, 0
        for j in range(side):
            row = source(side - self.base + j)
            near = inside(row)
            for i in range(self.slots):
                self.picks[i] = jnp.where((near == 1) & (seen == i), row - self.base, self.picks[i])
            seen = seen + near
        return self

    def rows(self, m, half):
        return pl.ds(pl.multiple_of((m * PAIR + half) * self.unit, self.unit), self.unit)

    def copy(self, src, dst, send, recv, row, col=None):
        return pltpu.make_async_remote_copy(
            src_ref=src, dst_ref=dst, send_sem=send, recv_sem=recv,
            device_id={"row": row, "col": self.c if col is None else col}, device_id_type=MESH,
        )

    def swap_copy(self, m):
        return self.copy(self.rb.at[1, self.rows(m, 1 - self.x)], self.swapped.at[m],
                         self.x_send.at[m], self.x_recv.at[m], self.base + self.beside)

    def hub_swap_copy(self, m):
        return self.copy(self.rb.at[1, self.rows(m, 1 - self.x)], self.pool[m].at[self.own],
                         self.x_send.at[m], self.up_recv.at[m, 2], self.hub + 1 - self.x)

    def up_copy(self, m):
        return self.copy(self.rb.at[1, self.rows(m, self.x)], self.pool[m].at[self.own],
                         self.up_send.at[m, 0], self.up_recv.at[m, 0], self.hub + self.x)

    def diagonal_copy(self, m):
        return self.copy(self.rb.at[1, self.rows(m, 1 - self.x)], self.pool[m].at[self.own],
                         self.up_send.at[m, 1], self.up_recv.at[m, 1], self.hub + 1 - self.x)

    def up_beside_copy(self, m):
        return self.copy(self.swapped.at[m], self.pool[m].at[self.beside],
                         self.up_send.at[m, 1], self.up_recv.at[m, 1], self.hub + self.x)

    def cross_copy(self, m):
        return self.copy(self.cross_out.at[m], self.crossed[m],
                         self.cross_send.at[m], self.cross_recv.at[m], self.other_hub + self.x)

    def deal_copy(self, m, j, half):
        return self.copy(self.deal_out.at[m, j], self.rb.at[2, self.rows(m, half)],
                         self.deal_send.at[m, j], self.deal_recv.at[m, half],
                         self.base + j, lax.rem(self.c + 1, self.nc))

    def send(self, q):
        @pl.when(self.inner)
        def _():
            for m in range(q * SUBS, (q + 1) * SUBS):
                self.hub_swap_copy(m).start()
                self.pool[m][self.own] = self.rb[1, self.rows(m, self.x), :]

        @pl.when(jnp.logical_not(self.inner))
        def _():
            for m in range(q * SUBS, (q + 1) * SUBS):
                if m < DIRECT:
                    self.up_copy(m).start()
                    self.diagonal_copy(m).start()
                else:
                    self.swap_copy(m).start()

    def gather(self, m):
        for k in range(3):
            self.copy(self.swapped.at[m], self.pool[m].at[0], self.x_send.at[m],
                      self.up_recv.at[m, k], self.r).wait_recv()
        for i in range(self.slots):
            self.cross_out[m, i] = self.pool[m][self.picks[i]]
        self.cross_copy(m).start()

    def deal(self, m):
        self.cross_copy(m).wait_recv()
        for j in range(self.side):
            near, here, there = self.deals[j]
            self.deal_out[m, j] = jnp.where(near == 1, self.pool[m][here], self.crossed[m][there])
            self.deal_copy(m, j, self.x).start()

    def forward(self):
        @pl.when(jnp.logical_not(self.inner))
        def _():
            for m in range(DIRECT, self.count):
                self.up_copy(m).start()
                self.swap_copy(m).wait_recv()
                self.up_beside_copy(m).start()

        @pl.when(self.inner)
        def _():
            for m in range(EARLY):
                self.gather(m)

    def arrive(self, q):
        steps = self.count + LAG
        done = [0] + [min(steps, (k + 1) * SUBS + LAG + AHEAD) for k in range(CHUNKS)]
        for fixed in range(CHUNKS):
            @pl.when((q == fixed) & self.inner)
            def _(fixed=fixed):
                for m in range(done[fixed], steps if fixed + 1 == CHUNKS else done[fixed + 1]):
                    if EARLY <= m < self.count:
                        self.gather(m)
                    if m >= LAG:
                        self.deal(m - LAG)

        def body(i, carry):
            for half in range(PAIR):
                self.deal_copy(q * SUBS + i, 0, half).wait_recv()
            return carry
        lax.fori_loop(0, SUBS, body, 0)

    def finish(self):
        def sent_swap(m, carry):
            self.copy(self.swapped.at[m], self.swapped.at[m], self.x_send.at[m], self.x_recv.at[m], self.r).wait_send()
            return carry
        @pl.when(self.inner)
        def _():
            lax.fori_loop(0, self.count, sent_swap, 0)

            def body(m, carry):
                self.copy(self.cross_out.at[m], self.cross_out.at[m],
                          self.cross_send.at[m], self.cross_recv.at[m], self.r).wait_send()
                for j in range(self.side):
                    self.copy(self.deal_out.at[m, j], self.deal_out.at[m, j],
                              self.deal_send.at[m, j], self.deal_recv.at[m, 0], self.r).wait_send()
                return carry
            lax.fori_loop(0, self.count, body, 0)

        @pl.when(jnp.logical_not(self.inner))
        def _():
            lax.fori_loop(DIRECT, self.count, sent_swap, 0)

            def body(m, carry):
                for k in range(2):
                    self.copy(self.swapped.at[m], self.swapped.at[m],
                              self.up_send.at[m, k], self.up_recv.at[m, 0], self.r).wait_send()
                return carry
            lax.fori_loop(0, self.count, body, 0)


def main_kernel(nr, nc, exchange, tiles, row_live, col_live, order, src_in, rec_in, src_out, rec_out, tile_out,
                tile, rb, stage, grad, half, half_t, row_mask,
                in_sem, ring_send, ring_recv, buffers):
    strata, block, width = tiles.shape
    rank = src_out.shape[1]
    chunk = rb.shape[2]
    chunks = width // chunk
    step_size = 1.0 / (width + 2 * rank)
    r = lax.axis_index("row")
    c = lax.axis_index("col")
    cn = lax.rem(c + 1, nc)
    rn = lax.rem(r + (c + 1) // nc, nr)
    cp = lax.rem(c + nc - 1, nc)

    tile_of = [tile.at[s] for s in range(strata - 1)] + [tile_out]
    loads = [
        pltpu.make_async_copy(rec_in, stage, in_sem.at[strata]),
        pltpu.make_async_copy(src_in, src_out, in_sem.at[strata + 1]),
    ] + [pltpu.make_async_copy(tiles.at[s], tile_of[s], in_sem.at[s]) for s in range(strata)]
    for load in loads[:3]:
        load.start()

    barrier = pltpu.get_barrier_semaphore()
    for k in range(nr):
        pl.semaphore_signal(barrier, inc=1, device_id={"row": k, "col": cp}, device_id_type=MESH)
    for k in range(1, nr):
        pl.semaphore_signal(
            barrier, inc=1, device_id={"row": lax.rem(r + k, nr), "col": c}, device_id_type=MESH
        )

    def ring_copy(s, q):
        lane = 0 if s == 0 else 1
        rows = pl.ds(q * rank, rank)
        return pltpu.make_async_remote_copy(
            src_ref=rb.at[s, rows], dst_ref=rb.at[s + 1, rows],
            send_sem=ring_send.at[lane, q], recv_sem=ring_recv.at[lane, q],
            device_id={"row": rn, "col": cn}, device_id_type=MESH,
        )

    moves = exchange(nr, nc, rank, chunk, chunks, rb, order, buffers)

    loads[0].wait()
    for q in range(chunks):
        rb[0, q * rank:(q + 1) * rank, :] = stage[q * chunk:(q + 1) * chunk, :].T
    loads[1].wait()

    for s in range(strata):
        lanes = row_live[s:s + 1, :].astype(F32)
        row_scale(lanes, row_mask, step_size)
        loads[s + 2].wait()
        if s == 0:
            for load in loads[3:]:
                load.start()
        for it in range(STEPS if s + 1 < strata else STEPS - 1):
            rounded_sources(src_out, lanes, half, half_t)

            def one(q, s=s, it=it):
                rows = pl.ds(pl.multiple_of(q * rank, rank), rank)
                cols = pl.ds(pl.multiple_of(q * chunk, chunk), chunk)
                if it == 0 and s == 2:
                    moves.arrive(q)
                elif it == 0:
                    ring_copy(s - 1, q).wait_recv()
                rec = rb[s, rows, :]
                rec_half = rec.astype(BF16)
                live = col_live[s:s + 1, cols].astype(F32)
                misfit = misfit_of(half, rec_half, tile_of[s][:, cols])
                grad_rec = jnp.dot(half_t[...], misfit, preferred_element_type=F32)
                updated = rec + (step_size * live) * grad_rec
                if s + 1 == strata:
                    rec_out[rows, :] = updated
                else:
                    rb[s, rows, :] = updated
                if it == STEPS - 1 and s in (0, 2):
                    ring_copy(s, q).start()
                if it == STEPS - 1 and s == 1:
                    for fixed in range(chunks):
                        pl.when(q == fixed)(functools.partial(moves.send, fixed))
                grad_src = source_gradient(misfit, rec_half, live)

                @pl.when(q == 0)
                def _():
                    grad[...] = grad_src

                @pl.when(q > 0)
                def _():
                    grad[...] += grad_src

            if it == STEPS - 1 and s == 0:
                pl.semaphore_wait(barrier, 2 * nr - 1)
            if it == 0 and s == 0:
                sweep(rb.at[0], rb.at[0], tile_of[0],
                      lambda q: col_live[0:1, q * chunk:(q + 1) * chunk].astype(F32),
                      half, half_t, grad, step_size)
            else:
                def body(q, carry):
                    one(q)
                    return carry
                lax.fori_loop(0, chunks, body, 0)
            if it == STEPS - 1 and s == 1:
                moves.forward()
            add_sources(src_out, src_out, row_mask, grad)
    for s in (0, 2):
        for q in range(chunks):
            ring_copy(s, q).wait_send()

    moves.finish()


def last_kernel(src_in, rec_in, tile, row_live, col_live, sources, receivers,
                half, half_t, grad, row_mask, rec_new, turned, src_new, sem):
    block, width = tile.shape
    rank = src_in.shape[1]
    chunk = rec_in.shape[1]
    chunks = width // chunk
    step_size = 1.0 / (width + 2 * rank)
    s = row_live.shape[0] - 1
    lanes = row_live[s:s + 1, :].astype(F32)
    rounded_sources(src_in, lanes, half, half_t)
    row_scale(lanes, row_mask, step_size)
    copies = []

    def done(q):
        rows = slice(q * chunk, (q + 1) * chunk)
        turned[rows, :] = rec_new[q * rank:(q + 1) * rank, :].T
        if q % 2 == 1:
            pair = pl.ds((q - 1) * chunk, 2 * chunk)
            copies.append(pltpu.make_async_copy(turned.at[pair], receivers.at[pair], sem.at[q // 2]))
            copies[-1].start()

    sweep(rec_in, rec_new, tile,
          lambda q: col_live[s:s + 1, q * chunk:(q + 1) * chunk].astype(F32),
          half, half_t, grad, step_size, done)
    add_sources(src_new, src_in, row_mask, grad)
    copies.append(pltpu.make_async_copy(src_new, sources, sem.at[chunks // 2]))
    copies[-1].start()
    for copy in copies:
        copy.wait()


def local(nr, nc, *args):
    if nr != LEVELS * PAIR:
        return run(nr, nc, Spread, 0, *args)
    source = args[3]
    side = nr // 2
    lower = jnp.arange(nr) < side
    direct = (lower & (source >= side)).astype(jnp.int32)
    shifted = (lower & ((source > side) | (source == 0))).astype(jnp.int32)
    field = 2 * nr
    crossing = jnp.sum(direct + field * shifted)

    def within(slots):
        return ((crossing + (nr - slots - 1) * (1 + field)) & (nr * (1 + field))) == 0

    relays = [functools.partial(run, nr, nc, Relay(slots), slots) for slots in (2, 3)]
    spread = functools.partial(run, nr, nc, Spread, 0)
    return lax.cond(
        within(2), relays[0], lambda *args: lax.cond(within(3), relays[1], spread, *args), *args
    )


def run(nr, nc, exchange, collective_id, tiles, row_live, col_live, row_order, source_init, receiver_init):
    strata, block, width = tiles.shape
    rank = source_init.shape[1]
    chunk = width // CHUNKS
    vmem = pl.BlockSpec(memory_space=pltpu.VMEM)
    anywhere = pl.BlockSpec(memory_space=pl.ANY)
    sources, receivers, tile = pl.pallas_call(
        functools.partial(main_kernel, nr, nc, exchange),
        out_shape=(
            pltpu.VMEM(source_init.shape, F32),
            pltpu.VMEM((CHUNKS * rank, chunk), F32),
            pltpu.VMEM((block, width), BF16),
        ),
        in_specs=[
            anywhere, vmem, vmem, pl.BlockSpec(memory_space=pltpu.SMEM), anywhere, anywhere,
        ],
        out_specs=(vmem, vmem, vmem),
        scratch_shapes=[
            pltpu.VMEM((strata - 1, block, width), BF16),
            pltpu.VMEM((strata, CHUNKS * rank, chunk), F32),
            pltpu.VMEM(receiver_init.shape, F32),
            pltpu.VMEM((block, rank), F32),
            pltpu.VMEM((block, rank), BF16),
            pltpu.VMEM((rank, block), BF16),
            pltpu.VMEM((block, LANES), F32),
            pltpu.SemaphoreType.DMA((strata + 2,)),
            pltpu.SemaphoreType.DMA((2, CHUNKS)),
            pltpu.SemaphoreType.DMA((2, CHUNKS)),
            exchange.scratch(nr, rank, chunk),
        ],
        compiler_params=pltpu.CompilerParams(
            collective_id=collective_id, has_side_effects=True, vmem_limit_bytes=56 * 1024 * 1024
        ),
    )(tiles, row_live, col_live, row_order, source_init, receiver_init)
    return pl.pallas_call(
        last_kernel,
        out_shape=(
            jax.ShapeDtypeStruct(source_init.shape, F32),
            jax.ShapeDtypeStruct(receiver_init.shape, F32),
        ),
        in_specs=[vmem] * 5,
        out_specs=(anywhere, anywhere),
        scratch_shapes=[
            pltpu.VMEM((block, rank), BF16),
            pltpu.VMEM((rank, block), BF16),
            pltpu.VMEM((block, rank), F32),
            pltpu.VMEM((block, LANES), F32),
            pltpu.VMEM((CHUNKS * rank, chunk), F32),
            pltpu.VMEM(receiver_init.shape, F32),
            pltpu.VMEM(source_init.shape, F32),
            pltpu.SemaphoreType.DMA((CHUNKS // 2 + 1,)),
        ],
        compiler_params=pltpu.CompilerParams(vmem_limit_bytes=40 * 1024 * 1024),
    )(sources, receivers, tile, row_live, col_live)


def solution(mesh):
    placed = (
        P(None, ("row", "col"), None),
        P(None, ("row", "col")),
        P(None, ("row", "col")),
        P(),
        P(("row", "col"), None),
        P(("row", "col"), None),
    )
    return jax.shard_map(
        functools.partial(local, mesh.shape["row"], mesh.shape["col"]),
        mesh=mesh,
        in_specs=placed,
        out_specs=(P(("row", "col"), None), P(("row", "col"), None)),
        check_vma=False,
    )
```
